256 devices in a mesh: section: 16 (over z_lo, x), tensor: 16 (over z_hi, y, core).
Axes of the slice: x: 4, y: 4, z: 8 (z_hi: 2, z_lo: 4; z = z_hi * 4 + z_lo), core: 2. Of those that a mesh axis runs over, the one named last changes fastest.
Arguments:
- hidden: bfloat16 [256, 8192], P(('section', 'tensor')), may hold values from -12 to 12
- weight: bfloat16 [131072, 8192], P(('section', 'tensor')), may hold values from -1 to 1
- targets: int32 [256], replicated, may hold values from 0 to 131071
- loss_grad: float32 [256], P(('section', 'tensor')), may hold values from 8 to 64
Outputs:
- token_loss: float32 [256], P(('section', 'tensor'))
- hidden_grad: bfloat16 [256, 8192], P(('section', 'tensor'))
The draws below stay inside these ranges and needn't reach their ends.
All inputs are finite; a program needn't handle non-finite values.
Results may differ from the reference program's by a relative error of at most 0.0039.
Values may be sent and summed in bfloat16 or wider, within the bound.
A program may use at most 64 MiB of HBM per device.

```python
import math
import jax
import jax.numpy as jnp
from jax import lax

D = 8192
TOKENS = 256
VOCAB = 131072


def weight_matrix(key):
    base_key = jax.random.fold_in(key, 11)
    keys = jax.random.split(base_key, 1)
    ramp = 1.0 + 0.25 * jnp.arange(VOCAB, dtype=jnp.float32) / VOCAB
    entries = jax.random.truncated_normal(keys[0], -6.0, 6.0, (VOCAB, D), jnp.float32)
    return (entries * ramp[:, None] * (3.0 / math.sqrt(D))).astype(jnp.bfloat16)


def draw_weight(key, part):
    return weight_matrix(key)


def draw_hidden(key, part):
    keys = jax.random.split(jax.random.fold_in(key, 23), 1)
    limit = 12.0 * max(1, 512 // D)
    values = jax.random.truncated_normal(keys[0], -6.0, 6.0, (TOKENS, D), jnp.float32)
    values = jnp.clip(values, -limit, limit)
    return values.astype(jnp.bfloat16)


def place_ends(array, stream_key, least, high):
    longest = array.shape.index(max(array.shape))
    spots = []
    for shift in (0, 1):
        where = [jax.random.randint(jax.random.fold_in(stream_key, axis), (), 0, length) for axis, length in enumerate(array.shape)]
        where[longest] = (where[longest] + shift) % array.shape[longest]
        spots.append(tuple(where))
    return array.at[spots[0]].set(least).at[spots[1]].set(high)


def steps_of(stream_key, dims, cuts, smallest, high):
    def one(dim, blocks):
        steps = jax.random.uniform(jax.random.fold_in(jax.random.fold_in(stream_key, 6), dim), (blocks,), jnp.float32, smallest / len(cuts), high / len(cuts))
        return jnp.repeat(jnp.exp(steps), dims[dim] // blocks).reshape((-1,) + (1,) * (len(dims) - dim - 1))

    level = one(*cuts[0])
    for cut in cuts[1:]:
        level = level * one(*cut)
    return level


def setup_inputs(seed: int = 0) -> dict:
    arg_keys = jax.random.split(jax.random.key(seed), 5)
    return {
        "hidden": draw_hidden(jax.random.fold_in(arg_keys[4], 71), 0),
        "weight": draw_weight(jax.random.fold_in(arg_keys[4], 71), 0),
        "targets": place_ends(jax.random.randint(arg_keys[2], (TOKENS,), 0, VOCAB), jax.random.fold_in(arg_keys[2], 1), 0, VOCAB - 1).astype(jnp.int32),
        "loss_grad": jnp.clip(jnp.exp(math.log(64.0) - 2.0794415 * jax.random.uniform(arg_keys[3], (TOKENS,), jnp.float32) ** steps_of(arg_keys[3], (TOKENS,), ((0, 256),), -0.2, 0.2)), 8.0, 64.0),
    }


def reference(hidden, weight, targets, loss_grad):
    logits = lax.dot_general(hidden, weight, (((1,), (1,)), ((), ())), preferred_element_type=jnp.float32)
    row_max = jnp.max(logits, axis=1)
    shifted = jnp.exp(logits - row_max[:, None])
    exp_total = jnp.sum(shifted, axis=1)
    target_logit = jnp.take_along_axis(logits, targets[:, None].astype(jnp.int32), axis=1)[:, 0]
    token_loss = row_max + jnp.log(exp_total) - target_logit
    columns = lax.broadcasted_iota(jnp.int32, logits.shape, 1)
    one_hot = (columns == targets[:, None].astype(jnp.int32)).astype(jnp.float32)
    probs_grad = (shifted / exp_total[:, None] - one_hot).astype(jnp.bfloat16)
    grad_sum = jnp.dot(probs_grad, weight, preferred_element_type=jnp.float32)
    hidden_grad = (loss_grad[:, None] * grad_sum).astype(jnp.bfloat16)
    return (token_loss, hidden_grad)
```

```python
import jax
import jax.numpy as jnp
from jax import lax
from jax.experimental import pallas as pl
from jax.experimental.pallas import tpu as pltpu
from jax.sharding import Mesh
from jax.sharding import PartitionSpec as P

AXES = ("zl", "x", "zh", "y", "c")
F32, BF16 = jnp.float32, jnp.bfloat16
QUARTER = 2048
LANES = 128


class Sems:
    def __init__(self, send, recv):
        self.send, self.recv, self.next = send, recv, 0

    def take(self):
        k = self.next
        self.next += 1
        return self.send.at[k], self.recv.at[k]


def kernel(
    h_ref, w_hbm, tgt_ref, lg_ref, loss_ref, grad_ref,
    wv, row_f, row_b, got, wide, hid, logits, pt, stat, st1, st2, own_sum, give, take,
    ub, vb_opp, vb_all, ua, va_opp, va_all, acc_a, rows_out, rows_b, rows_in,
    w_sem, send_sem, recv_sem,
):
    zl, x, zh, y, c = (lax.axis_index(a) for a in AXES)
    z = zh * 4 + zl
    sems = Sems(send_sem, recv_sem)
    pending = []

    def device(x_, y_, z_, c_):
        return (lax.rem(z_, 4), x_, lax.div(z_, 4), y_, c_)

    def send(src, dst, to):
        s, r = sems.take()
        copy = pltpu.make_async_remote_copy(
            src_ref=src, dst_ref=dst, send_sem=s, recv_sem=r,
            device_id=to, device_id_type=pl.DeviceIdType.MESH,
        )
        copy.start()
        pending.append(copy)
        return copy

    up = {"x": lax.rem(x + 1, 4), "y": lax.rem(y + 1, 4)}
    opp = {"x": lax.rem(x + 2, 4), "y": lax.rem(y + 2, 4)}
    down = {"x": lax.rem(x + 3, 4), "y": lax.rem(y + 3, 4)}
    here = {"x": x, "y": y}

    def to_up(axis):
        return device(up["x"] if axis == "x" else x, up["y"] if axis == "y" else y, z, c)

    def to_down(axis):
        return device(down["x"] if axis == "x" else x, down["y"] if axis == "y" else y, z, c)

    partner = device(x, y, z, 1 - c)
    column = [(dz, dc) for dz in range(8) for dc in range(2) if (dz, dc) != (0, 0)]
    plane = [(dx, dy) for dx in range(4) for dy in range(4) if (dx, dy) != (0, 0)]

    def in_column(dz, dc):
        return lax.rem(z + dz, 8), lax.rem(c + dc, 2)

    def in_plane(dx, dy):
        return lax.rem(x + dx, 4), lax.rem(y + dy, 4)

    w_copies = [
        pltpu.make_async_copy(
            w_hbm.at[:, pl.ds(q * QUARTER, QUARTER)], wv.at[:, pl.ds(q * QUARTER, QUARTER)], w_sem.at[q]
        )
        for q in range(4)
    ]
    for copy in w_copies:
        copy.start()

    barrier = pltpu.get_barrier_semaphore()
    for dz, dc in column:
        z_, c_ = in_column(dz, dc)
        pl.semaphore_signal(barrier, inc=1, device_id=device(x, y, z_, c_), device_id_type=pl.DeviceIdType.MESH)
    for dx, dy in plane:
        x_, y_ = in_plane(dx, dy)
        pl.semaphore_signal(barrier, inc=1, device_id=device(x_, y_, z, c), device_id_type=pl.DeviceIdType.MESH)

    for k in range(64):
        row_f[pl.ds(k, 1), :] = h_ref[:, pl.ds(k * LANES, LANES)].astype(F32)
    row_b[...] = row_f[...].astype(BF16)
    me = z * 2 + c

    pl.semaphore_wait(barrier, len(column) + len(plane))

    arrivals = []
    for dz, dc in column:
        z_, c_ = in_column(dz, dc)
        arrivals.append(
            send(row_b.at[pl.ds(pl.multiple_of(c_ * 32, 32), 32)], got.at[me], device(x, y, z_, c_))
        )
    got[me] = row_b[pl.ds(pl.multiple_of(c * 32, 32), 32), :]
    for copy in arrivals:
        copy.wait_recv()
    wide[...] = got[...].astype(F32)
    for k in range(32):
        hid[2 * c + k // 16, y, x, :, pl.ds((k % 16) * LANES, LANES)] = wide[:, k, :].astype(BF16)

    def block(part, b_index, a_index):
        return (b_index, a_index) if part == 0 else (a_index, b_index)

    first = ("x", "y")
    second = ("y", "x")
    half_rows = QUARTER // 2
    gathers = []
    from_partner = []

    def share(part, index):
        ref = hid.at[2 * c + part, index[0], index[1]]
        from_partner.append(send(ref, ref, partner))

    for part in range(2):
        a, b = first[part], second[part]
        index = block(part, here[b], here[a])
        ref = hid.at[2 * c + part, index[0], index[1]]
        g = {"a": {}, "b": {}}
        g["a"]["from_down"] = send(ref, ref, to_up(a))
        g["a"]["from_up"] = send(ref, ref, to_down(a))
        gathers.append(g)

    def second_axis(part, rel, a_index):
        b = second[part]
        index = block(part, here[b], a_index)
        ref = hid.at[2 * c + part, index[0], index[1]]
        gathers[part]["b"][rel, "from_down"] = send(ref, ref, to_up(b))
        gathers[part]["b"][rel, "from_up"] = send(ref, ref, to_down(b))
        share(part, index)

    def halves(ref, k):
        return ref.at[:, pl.ds(k * half_rows, half_rows)]

    for part in range(2):
        second_axis(part, "own", here[first[part]])
    for part in range(2):
        a, b = first[part], second[part]
        q = 2 * c + part
        g = gathers[part]["a"]
        g["from_down"].wait_recv()
        index = block(part, here[b], down[a])
        ref = halves(hid.at[q, index[0], index[1]], 0)
        g["opp0"] = send(ref, ref, to_up(a))
        g["from_up"].wait_recv()
        index = block(part, here[b], up[a])
        ref = halves(hid.at[q, index[0], index[1]], 1)
        g["opp1"] = send(ref, ref, to_down(a))
    for part in range(2):
        a = first[part]
        second_axis(part, "down", down[a])
        second_axis(part, "up", up[a])
    for part in range(2):
        a = first[part]
        g = gathers[part]["a"]
        g["opp0"].wait_recv()
        g["opp1"].wait_recv()
        second_axis(part, "opp", opp[a])
    rels = {"own": here, "down": down, "up": up, "opp": opp}
    for rel in ("own", "down", "up", "opp"):
        for part in range(2):
            a, b = first[part], second[part]
            g = gathers[part]["b"]
            q = 2 * c + part
            for side, place, to in (("from_down", down, to_up), ("from_up", up, to_down)):
                g[rel, side].wait_recv()
                index = block(part, place[b], rels[rel][a])
                ref = hid.at[q, index[0], index[1]]
                if (rel in ("own", "up")) == (side == "from_down"):
                    g[rel, "opp"] = send(ref, ref, to(b))
                share(part, index)
    for rel in ("own", "down", "up", "opp"):
        for part in range(2):
            a, b = first[part], second[part]
            gathers[part]["b"][rel, "opp"].wait_recv()
            share(part, block(part, opp[b], rels[rel][a]))
    for copy in from_partner:
        copy.wait_recv()
    for copy in w_copies:
        copy.wait()

    logits[...] = jnp.zeros_like(logits)

    def logits_step(k, _):
        q, m = lax.div(k, 2), lax.rem(k, 2)
        rows = pl.ds(pl.multiple_of(m * 256, 256), 256)
        logits[rows, :] += lax.dot_general(
            wv[rows, pl.ds(pl.multiple_of(q * QUARTER, QUARTER), QUARTER)],
            hid[q].reshape(256, QUARTER),
            (((1,), (1,)), ((), ())),
            preferred_element_type=F32,
        )
        return 0

    lax.fori_loop(0, 8, logits_step, 0)

    lt = logits[...]
    vocab_dev = lt.shape[0]
    offset = ((zl * 4 + x) * 16 + zh * 8 + y * 2 + c) * vocab_dev
    columns = lax.broadcasted_iota(jnp.int32, (vocab_dev, 256), 0) + offset
    mask = columns == tgt_ref[...]
    local_max = jnp.max(lt, axis=0, keepdims=True)
    local_total = jnp.sum(jnp.exp(lt - local_max), axis=0, keepdims=True)
    local_target = jnp.sum(jnp.where(mask, lt, 0.0), axis=0, keepdims=True)

    def put(ref_rows, values):
        for k, v in enumerate(values):
            for j in range(2):
                ref_rows(2 * k + j, v[:, j * LANES : (j + 1) * LANES])

    def combined(ref):
        v = ref[...]
        mx = jnp.max(v[:, 0:2], axis=0)
        total = jnp.sum(v[:, 2:4] * jnp.exp(v[:, 0:2] - mx[None]), axis=0)
        target = jnp.sum(v[:, 4:6], axis=0)
        return mx, total, target

    stat[...] = jnp.zeros_like(stat)
    for k, v in enumerate((local_max, local_total, local_target)):
        for j in range(2):
            stat[0, pl.ds(2 * k + j, 1), :] = v[:, j * LANES : (j + 1) * LANES]
    arrivals = []
    for dz, dc in column:
        z_, c_ = in_column(dz, dc)
        arrivals.append(send(stat.at[0], st1.at[me], device(x, y, z_, c_)))
    st1[me] = stat[0]
    for copy in arrivals:
        copy.wait_recv()
    for k, v in enumerate(combined(st1)):
        stat[1, pl.ds(2 * k, 2), :] = v
    spot = y * 4 + x
    arrivals = []
    for dx, dy in plane:
        x_, y_ = in_plane(dx, dy)
        arrivals.append(send(stat.at[1], st2.at[spot], device(x_, y_, z, c)))
    st2[spot] = stat[1]
    for copy in arrivals:
        copy.wait_recv()
    mx, total, target = combined(st2)
    rows2 = lax.broadcasted_iota(jnp.int32, (2, LANES), 0) * LANES + lax.broadcasted_iota(jnp.int32, (2, LANES), 1)
    mine = spot * 16 + me
    loss_ref[0, 0] = jnp.sum(jnp.where(rows2 == mine, mx + jnp.log(total) - target, 0.0))
    inverse = 1.0 / total

    def flat(v):
        return jnp.concatenate([v[0:1], v[1:2]], axis=1)

    probs = jnp.exp(logits[...] - flat(mx)) * flat(inverse) - jnp.where(mask, 1.0, 0.0)
    pt[...] = probs.T.astype(BF16)

    tile = 512

    def product(q, n):
        start = pl.multiple_of(q * QUARTER + n * tile, tile)
        return jnp.dot(pt[...], wv[:, pl.ds(start, tile)], preferred_element_type=F32).reshape(4, 4, 16, tile)

    swaps = []
    for part in range(2):
        q = 2 * (1 - c) + part

        def give_step(n, _, q=q, part=part):
            give[part, :, :, :, pl.ds(pl.multiple_of(n * tile, tile), tile)] = product(q, n).astype(BF16)
            return 0

        lax.fori_loop(0, QUARTER // tile, give_step, 0)
        swaps.append(send(give.at[part], take.at[part], partner))
    for part in range(2):
        q = 2 * c + part

        def own_step(n, _, q=q, part=part):
            own_sum[part, :, :, :, pl.ds(pl.multiple_of(n * tile, tile), tile)] = product(q, n)
            return 0

        lax.fori_loop(0, QUARTER // tile, own_step, 0)

    def chip_sum(part, index):
        return own_sum[part, index[0], index[1]] + take[part, index[0], index[1]].astype(F32)

    order = ("own", "up", "down", "opp")
    low, high = ("own", "up"), ("down", "opp")
    reds = [dict() for _ in range(2)]
    for part in range(2):
        a, b = first[part], second[part]
        swaps[part].wait_recv()
        r = reds[part]
        for rel in order:
            ub[part, 0, order.index(rel)] = chip_sum(part, block(part, opp[b], rels[rel][a])).astype(BF16)
            k = order.index(rel) % 2
            if rel in low:
                r["opp", rel] = send(ub.at[part, 0, order.index(rel)], vb_opp.at[part, order.index(rel)], to_up(b))
            else:
                r["opp", rel] = send(ub.at[part, 0, order.index(rel)], vb_opp.at[part, order.index(rel)], to_down(b))
    for part in range(2):
        a, b = first[part], second[part]
        r = reds[part]
        for rel in order:
            k = order.index(rel)
            if rel in high:
                slot, place, to = 0, up, to_up
            else:
                slot, place, to = 1, down, to_down
            ub[part, 1 + slot, k] = chip_sum(part, block(part, place[b], rels[rel][a])).astype(BF16)
            r[slot, rel] = send(ub.at[part, 1 + slot, k], vb_all.at[part, slot, k], to(b))
    for rel in order:
        for part in range(2):
            a, b = first[part], second[part]
            r = reds[part]
            k = order.index(rel)
            r["opp", rel].wait_recv()
            if rel in low:
                slot, place, to = 0, up, to_up
            else:
                slot, place, to = 1, down, to_down
            ub[part, 1 + slot, k] = (
                chip_sum(part, block(part, place[b], rels[rel][a])) + vb_opp[part, k].astype(F32)
            ).astype(BF16)
            r[slot, rel] = send(ub.at[part, 1 + slot, k], vb_all.at[part, slot, k], to(b))

    def line_sum(part, rel):
        a, b = first[part], second[part]
        k = order.index(rel)
        for slot in range(2):
            reds[part][slot, rel].wait_recv()
        return (
            chip_sum(part, block(part, here[b], rels[rel][a]))
            + vb_all[part, 0, k].astype(F32)
            + vb_all[part, 1, k].astype(F32)
        )

    half = QUARTER // 2
    for part in range(2):
        a = first[part]
        r = reds[part]
        ua[part, 0] = line_sum(part, "opp").astype(BF16)
        r["a_opp0"] = send(halves(ua.at[part, 0], 0), va_opp.at[part, 0], to_up(a))
        r["a_opp1"] = send(halves(ua.at[part, 0], 1), va_opp.at[part, 1], to_down(a))
    keep = {}
    for part in range(2):
        a = first[part]
        r = reds[part]
        for slot, rel, to in ((0, "up", to_up), (1, "down", to_down)):
            keep[part, slot] = line_sum(part, rel)
            own_half = 1 - slot
            ua[part, 1 + slot, :, pl.ds(own_half * half, half)] = keep[part, slot][
                :, own_half * half : (own_half + 1) * half
            ].astype(BF16)
            r["a", slot, own_half] = send(
                halves(ua.at[part, 1 + slot], own_half), va_all.at[part, slot, own_half], to(a)
            )
    for part in range(2):
        a = first[part]
        r = reds[part]
        for slot, to in ((0, to_up), (1, to_down)):
            r[f"a_opp{slot}"].wait_recv()
            ua[part, 1 + slot, :, pl.ds(slot * half, half)] = (
                keep[part, slot][:, slot * half : (slot + 1) * half] + va_opp[part, slot].astype(F32)
            ).astype(BF16)
            r["a", slot, slot] = send(halves(ua.at[part, 1 + slot], slot), va_all.at[part, slot, slot], to(a))
    for part in range(2):
        acc_a[part] = line_sum(part, "own")
    for part in range(2):
        r = reds[part]
        for k in range(2):
            for slot in range(2):
                r["a", slot, k].wait_recv()
            acc_a[part, :, pl.ds(k * half, half)] += va_all[part, 0, k].astype(F32) + va_all[part, 1, k].astype(F32)

    for k in range(32):
        rows_out[:, k, :] = acc_a[k // 16, :, pl.ds((k % 16) * LANES, LANES)]
    rows_b[...] = rows_out[...].astype(BF16)
    arrivals = []
    for dz, dc in column:
        z_, c_ = in_column(dz, dc)
        arrivals.append(send(rows_b.at[z_ * 2 + c_], rows_in.at[c, z], device(x, y, z_, c_)))
    rows_in[c, z] = jnp.zeros((32, LANES), BF16)
    for copy in arrivals:
        copy.wait_recv()
    summed = jnp.sum(rows_in[...].astype(F32), axis=1)
    row_f[...] = summed.reshape(64, LANES)
    row_f[pl.ds(pl.multiple_of(c * 32, 32), 32), :] += rows_out[me]
    grad_ref[...] = (row_f[...] * lg_ref[0, 0]).astype(BF16)

    for copy in pending:
        copy.wait_send()


COPIES = 512


def shards(hidden, weight, targets, loss_grad):
    order = targets.reshape(4, 4, 2, 4, 2).transpose(3, 1, 2, 0, 4).reshape(1, 256)
    vmem = pltpu.VMEM
    loss, grad = pl.pallas_call(
        kernel,
        out_shape=(jax.ShapeDtypeStruct((1, 1), F32), jax.ShapeDtypeStruct((64, LANES), BF16)),
        in_specs=[
            pl.BlockSpec(memory_space=pltpu.VMEM),
            pl.BlockSpec(memory_space=pl.ANY),
            pl.BlockSpec(memory_space=pltpu.VMEM),
            pl.BlockSpec(memory_space=pltpu.SMEM),
        ],
        out_specs=(pl.BlockSpec(memory_space=pltpu.SMEM), pl.BlockSpec(memory_space=pltpu.VMEM)),
        scratch_shapes=[
            vmem(weight.shape, BF16),
            vmem((64, LANES), F32),
            vmem((64, LANES), BF16),
            vmem((16, 32, LANES), BF16),
            vmem((16, 32, LANES), F32),
            vmem((4, 4, 4, 16, QUARTER), BF16),
            vmem((512, 256), F32),
            vmem((256, 512), BF16),
            vmem((2, 8, LANES), F32),
            vmem((16, 8, LANES), F32),
            vmem((16, 8, LANES), F32),
            vmem((2, 4, 4, 16, QUARTER), F32),
            vmem((2, 4, 4, 16, QUARTER), BF16),
            vmem((2, 4, 4, 16, QUARTER), BF16),
            vmem((2, 3, 4, 16, QUARTER), BF16),
            vmem((2, 4, 16, QUARTER), BF16),
            vmem((2, 2, 4, 16, QUARTER), BF16),
            vmem((2, 3, 16, QUARTER), BF16),
            vmem((2, 2, 16, QUARTER // 2), BF16),
            vmem((2, 2, 2, 16, QUARTER // 2), BF16),
            vmem((2, 16, QUARTER), F32),
            vmem((16, 32, LANES), F32),
            vmem((16, 32, LANES), BF16),
            vmem((2, 8, 32, LANES), BF16),
            pltpu.SemaphoreType.DMA((4,)),
            pltpu.SemaphoreType.DMA((COPIES,)),
            pltpu.SemaphoreType.DMA((COPIES,)),
        ],
        compiler_params=pltpu.CompilerParams(
            collective_id=0, has_side_effects=True, vmem_limit_bytes=60 * 1024 * 1024
        ),
    )(hidden, weight, order, loss_grad.reshape(1, 1))
    return loss.reshape(1), grad.reshape(1, 8192)


def solution(mesh):
    finer = Mesh(mesh.devices.reshape(4, 4, 2, 4, 2), AXES)
    whole = ("zl", "x", "zh", "y", "c")
    return jax.shard_map(
        shards,
        mesh=finer,
        in_specs=(P(whole, None), P(whole, None), P(), P(whole)),
        out_specs=(P(whole), P(whole, None)),
        check_vma=False,
    )
```

```python
import jax
import jax.numpy as jnp
from jax import lax
from jax.experimental import pallas as pl
from jax.experimental.pallas import tpu as pltpu
from jax.sharding import Mesh
from jax.sharding import PartitionSpec as P

AXES = ("zl", "x", "zh", "y", "c")
F32, BF16 = jnp.float32, jnp.bfloat16
SLAB = 2048
PART = 1024
HALF = 512
LANES = 128
SENDS, RECVS = 24, 132
MESH = pl.DeviceIdType.MESH


def kernel(
    h_ref, w_hbm, tgt_ref, lg_ref, loss_ref, grad_ref,
    wv, wp, row_f, row_b, got, wide, hid, logits, logits_p, pt, stz, stz1, stz2, stt, stt1, stt2,
    own_sum, ub, vb_opp, vb_all, keep, ua, va_opp, va_all, acc, rows_out, rows_b, rows_in,
    w_sem, send_sem, recv_sem,
):
    zl, x, zh, y, c = (lax.axis_index(a) for a in AXES)
    z = zh * 4 + zl
    me, spot = z * 2 + c, y * 4 + x
    counts = {"send": 0, "recv": 0}
    ends = []

    def new(kind, sem):
        counts[kind] += 1
        return sem.at[counts[kind] - 1]

    def new_recv():
        return new("recv", recv_sem)

    def new_send(ref):
        s = new("send", send_sem)
        ends.append((s, ref))
        return s

    def take(sem, ref):
        pltpu.make_async_copy(ref, ref, sem).wait()

    def send(src, dst, to, s, r):
        pltpu.make_async_remote_copy(
            src_ref=src, dst_ref=dst, send_sem=s, recv_sem=r, device_id=to, device_id_type=MESH
        ).start()

    def device(x_, y_, z_, c_):
        return (lax.rem(z_, 4), x_, lax.div(z_, 4), y_, c_)

    up = {"x": lax.rem(x + 1, 4), "y": lax.rem(y + 1, 4)}
    opp = {"x": lax.rem(x + 2, 4), "y": lax.rem(y + 2, 4)}
    down = {"x": lax.rem(x + 3, 4), "y": lax.rem(y + 3, 4)}
    here = {"x": x, "y": y}
    rels = {"own": here, "down": down, "up": up, "opp": opp}
    first, second = ("x", "y"), ("y", "x")
    order = ("own", "up", "down", "opp")

    def to_up(axis):
        return device(up["x"] if axis == "x" else x, up["y"] if axis == "y" else y, z, c)

    def to_down(axis):
        return device(down["x"] if axis == "x" else x, down["y"] if axis == "y" else y, z, c)

    partner = device(x, y, z, 1 - c)
    column = [(dz, dc) for dz in (4, 3, 5, 2, 6, 1, 7, 0) for dc in range(2) if (dz, dc) != (0, 0)]
    plane = [(dx, dy) for dx in (2, 1, 3, 0) for dy in (2, 1, 3, 0) if (dx, dy) != (0, 0)]

    def in_column(dz, dc):
        return lax.rem(z + dz, 8), lax.rem(c + dc, 2)

    def in_plane(dx, dy):
        return lax.rem(x + dx, 4), lax.rem(y + dy, 4)

    def block(part, b_index, a_index):
        return (b_index, a_index) if part == 0 else (a_index, b_index)

    halfway = SLAB * 2
    w_copies = []
    for k, half in enumerate((1 - c, c)):
        cols = pl.ds(pl.multiple_of(half * halfway, halfway), halfway)
        w_copies.append(pltpu.make_async_copy(w_hbm.at[:, cols], wv.at[:, cols], w_sem.at[k]))
        w_copies[-1].start()

    barrier = pltpu.get_barrier_semaphore()
    for dz, dc in column:
        z_, c_ = in_column(dz, dc)
        pl.semaphore_signal(barrier, inc=1, device_id=device(x, y, z_, c_), device_id_type=MESH)
    for dx, dy in plane:
        x_, y_ = in_plane(dx, dy)
        pl.semaphore_signal(barrier, inc=1, device_id=device(x_, y_, z, c), device_id_type=MESH)

    for k in range(64):
        row_f[pl.ds(k, 1), :] = h_ref[:, pl.ds(k * LANES, LANES)].astype(F32)
    row_b[...] = row_f[...].astype(BF16)

    chip_base = ((zl * 4 + x) * 16 + zh * 8 + y * 2) * 512
    rel = tgt_ref[...] - chip_base
    near = jnp.logical_and(rel >= 0, rel < 1024)
    high = jnp.where(near, lax.shift_right_logical(rel, 4), 128)
    low = jnp.where(near, jnp.bitwise_and(rel, 15), 0)
    digit = lax.broadcasted_iota(jnp.int32, (16, 256), 0)
    digits = jnp.where(digit == 0, high, jnp.where(digit == 1, low, 0)).astype(F32).astype(BF16)
    r = lax.broadcasted_iota(jnp.int32, (256, 256), 1)
    t = lax.broadcasted_iota(jnp.int32, (256, 256), 0)
    bits = jnp.bitwise_and
    shift = lax.shift_right_logical
    token = (
        bits(shift(r, 1), 3) * 64 + bits(shift(r, 4), 3) * 16 + bits(shift(r, 3), 1) * 8 + shift(r, 6) * 2 + bits(r, 1)
    )
    moves = jnp.where(t == token, 1.0, 0.0).astype(BF16)
    placed = jnp.dot(digits, moves, preferred_element_type=F32)
    chip_row = (placed[0:1] * 16.0 + placed[1:2]).astype(jnp.int32)

    pl.semaphore_wait(barrier, len(column) + len(plane))

    col_recv = []
    for s in range(2):
        ss, rr = new_send(got.at[s, pl.ds(0, 15)]), new_recv()
        for dz, dc in column:
            z_, c_ = in_column(dz, dc)
            rows = pl.ds(pl.multiple_of(c_ * 32 + s * 16, 16), 16)
            send(row_b.at[rows], got.at[s, me], device(x, y, z_, c_), ss, rr)
        got[s, me] = row_b[pl.ds(pl.multiple_of(c * 32 + s * 16, 16), 16), :]
        col_recv.append(rr)

    a_send = new_send(hid.at[pl.ds(0, 3), 0, pl.ds(0, 2)])
    b_send = new_send(hid.at[pl.ds(0, 3), pl.ds(0, 2)])
    share_send = new_send(hid.at[pl.ds(0, 2)])
    share_recv = [new_recv() for _ in range(2)]
    w_send, w_recv = new_send(wp), new_recv()
    a_recv = {(s, p, k): new_recv() for s in range(2) for p in range(2) for k in ("down", "up", "opp")}
    b_recv = {
        (s, p, side, k): new_recv()
        for s in range(2) for p in range(2) for side in ("down", "up") for k in ("own", "next", "opp", "far")
    }

    def blk(s, p, index, cols=None):
        lo, n = (p * PART, PART) if cols is None else (p * PART + cols * HALF, HALF)
        return hid.at[2 * c + s, index[0], index[1], :, pl.ds(lo, n)]

    def share(s, p, index):
        ref = blk(s, p, index)
        send(ref, ref, partner, share_send, share_recv[s])

    def w_piece(k):
        src = wv.at[pl.ds(64 * k, 64), pl.ds(pl.multiple_of((1 - c) * halfway, halfway), halfway)]
        send(src, wp.at[pl.ds(64 * k, 64)], partner, w_send, w_recv)

    def second_axis(s, p, name, group):
        b = second[p]
        index = block(p, here[b], rels[name][first[p]])
        ref = blk(s, p, index)
        send(ref, ref, to_up(b), b_send, b_recv[s, p, "down", group])
        send(ref, ref, to_down(b), b_send, b_recv[s, p, "up", group])
        share(s, p, index)

    def step_c(s):
        take(col_recv[s], got.at[s, pl.ds(0, 15)])
        wide[...] = got[s].astype(F32)
        for k in range(16):
            hid[2 * c + s, y, x, :, pl.ds(k * LANES, LANES)] = wide[:, k, :].astype(BF16)
        for p in range(2):
            a = first[p]
            ref = blk(s, p, (y, x))
            send(ref, ref, to_up(a), a_send, a_recv[s, p, "down"])
            send(ref, ref, to_down(a), a_send, a_recv[s, p, "up"])
        for p in range(2):
            second_axis(s, p, "own", "own")

    def step_a1(s):
        for p in range(2):
            a, b = first[p], second[p]
            for k, (name, to) in enumerate((("down", to_up), ("up", to_down))):
                index = block(p, here[b], rels[name][a])
                take(a_recv[s, p, name], blk(s, p, index))
                ref = blk(s, p, index, k)
                send(ref, ref, to(a), a_send, a_recv[s, p, "opp"])
        for p in range(2):
            for name in ("down", "up"):
                second_axis(s, p, name, "next")

    def step_a2(s):
        for p in range(2):
            take(a_recv[s, p, "opp"], blk(s, p, block(p, here[second[p]], opp[first[p]])))
            second_axis(s, p, "opp", "opp")

    def step_b(s, group):
        names = {"own": ("own",), "next": ("down", "up"), "opp": ("opp",)}[group]
        for p in range(2):
            a, b = first[p], second[p]
            for side, place, to in (("down", down, to_up), ("up", up, to_down)):
                refs = [(n, block(p, place[b], rels[n][a])) for n in names]
                some = hid.at[2 * c + s, 0, pl.ds(0, len(names)), :, pl.ds(0, PART)]
                take(b_recv[s, p, side, group], some)
                for n, index in refs:
                    if (n in ("own", "up")) == (side == "down"):
                        ref = blk(s, p, index)
                        send(ref, ref, to(b), b_send, b_recv[s, p, side, "far"])
                for n, index in refs:
                    share(s, p, index)

    def step_far(s):
        for p in range(2):
            a, b = first[p], second[p]
            for side, names in (("down", ("own", "up")), ("up", ("down", "opp"))):
                take(b_recv[s, p, side, "far"], hid.at[2 * c + s, 0, pl.ds(0, 2), :, pl.ds(0, PART)])
                for n in names:
                    share(s, p, block(p, opp[b], rels[n][a]))

    def step_logits(s, half, start=False):
        v = half * 2 + s
        part = lax.dot_general(
            wv[:, pl.ds(pl.multiple_of(v * SLAB, SLAB), SLAB)],
            hid[v].reshape(256, SLAB),
            (((1,), (1,)), ((), ())),
            preferred_element_type=F32,
        )
        if start:
            logits[...] = part
        else:
            logits[...] += part

    w_copies[0].wait()
    step_c(0)
    step_a1(0)
    step_c(1)
    w_piece(0)
    step_a2(0)
    step_b(0, "own")
    w_piece(1)
    step_a1(1)
    w_piece(2)
    step_b(0, "next")
    w_piece(3)
    step_a2(1)
    step_b(0, "opp")
    w_piece(4)
    step_b(1, "own")
    w_piece(5)
    w_copies[1].wait()
    step_far(0)
    w_piece(6)
    step_b(1, "next")
    w_piece(7)
    step_logits(0, c, True)
    step_b(1, "opp")
    take(share_recv[0], hid.at[0])
    step_logits(0, 1 - c)
    step_far(1)
    step_logits(1, c)
    take(share_recv[1], hid.at[0])
    step_logits(1, 1 - c)

    swap_send, swap_recv = new_send(logits), new_recv()
    send(logits, logits_p, partner, swap_send, swap_recv)
    lt = logits[...]
    vocab_row = lax.broadcasted_iota(jnp.int32, (512, 256), 0)
    mask = vocab_row + c * 512 == chip_row
    local_max = jnp.max(lt, axis=0, keepdims=True)
    local_total = jnp.sum(jnp.exp(lt - local_max), axis=0, keepdims=True)

    def put(ref, row, v):
        for j in range(2):
            ref[0, pl.ds(row + j, 1), :] = v[:, j * LANES : (j + 1) * LANES]

    def over_column(src, dst):
        ss, rr = new_send(dst.at[pl.ds(0, 15)]), new_recv()
        for dz, dc in column:
            z_, c_ = in_column(dz, dc)
            send(src.at[0], dst.at[me], device(x, y, z_, c_), ss, rr)
        dst[me] = src[0]
        return rr

    def over_plane(src, dst):
        ss, rr = new_send(dst.at[pl.ds(0, 15)]), new_recv()
        for dx, dy in plane:
            x_, y_ = in_plane(dx, dy)
            send(src.at[1], dst.at[spot], device(x_, y_, z, c), ss, rr)
        dst[spot] = src[1]
        return rr

    def combined(ref):
        v = ref[...]
        mx = jnp.max(v[:, 0:2], axis=0)
        total = jnp.sum(v[:, 2:4] * jnp.exp(v[:, 0:2] - mx[None]), axis=0)
        return mx, total

    put(stz, 0, local_max)
    put(stz, 2, local_total)
    rr = over_column(stz, stz1)
    put(stt, 0, jnp.sum(jnp.where(mask, lt, 0.0), axis=0, keepdims=True))
    tt = over_column(stt, stt1)
    take(rr, stz1.at[pl.ds(0, 15)])
    for k, v in enumerate(combined(stz1)):
        stz[1, pl.ds(2 * k, 2), :] = v
    rr = over_plane(stz, stz2)
    take(tt, stt1.at[pl.ds(0, 15)])
    stt[1] = jnp.sum(stt1[...], axis=0)
    tt = over_plane(stt, stt2)
    take(swap_recv, logits_p)
    take(w_recv, wp)
    take(rr, stz2.at[pl.ds(0, 15)])
    mx, total = combined(stz2)

    def flat(v):
        return jnp.concatenate([v[0:1], v[1:2]], axis=1)

    mx_row, inverse = flat(mx), flat(1.0 / total)
    for k, (ref, half) in enumerate(((logits, c), (logits_p, 1 - c))):
        here_mask = vocab_row + half * 512 == chip_row
        probs = jnp.exp(ref[...] - mx_row) * inverse - jnp.where(here_mask, 1.0, 0.0)
        pt[k] = probs.T.astype(BF16)

    low_names, high_names = ("own", "up"), ("down", "opp")
    ub_send, ua_send = new_send(ub), new_send(ua)
    rb = {
        (s, p, k): new_recv() for s in range(2) for p in range(2)
        for k in ("opp0", "opp1", (0, "plain"), (0, "sum"), (1, "plain"), (1, "sum"))
    }
    ra = {
        (s, p, k): new_recv() for s in range(2) for p in range(2)
        for k in ("opp0", "opp1", (0, "plain"), (0, "sum"), (1, "plain"), (1, "sum"))
    }

    def product(s, p):
        def tile(n, _):
            at = s * SLAB + p * PART + n * HALF
            mine = pl.ds(pl.multiple_of(c * halfway + at, HALF), HALF)
            theirs = pl.ds(pl.multiple_of(at, HALF), HALF)
            out = jnp.dot(pt[0], wv[:, mine], preferred_element_type=F32) + jnp.dot(
                pt[1], wp[:, theirs], preferred_element_type=F32
            )
            own_sum[s, p, :, :, :, pl.ds(pl.multiple_of(n * HALF, HALF), HALF)] = out.reshape(4, 4, 16, HALF)
            return 0

        lax.fori_loop(0, PART // HALF, tile, 0)

    def mine_of(s, p, index):
        return own_sum[s, p, index[0], index[1]]

    def red_far(s, p):
        a, b = first[p], second[p]
        for n in order:
            k = order.index(n)
            ub[s, p, 0, k] = mine_of(s, p, block(p, opp[b], rels[n][a])).astype(BF16)
            if n in low_names:
                send(ub.at[s, p, 0, k], vb_opp.at[s, p, k], to_up(b), ub_send, rb[s, p, "opp0"])
            else:
                send(ub.at[s, p, 0, k], vb_opp.at[s, p, k], to_down(b), ub_send, rb[s, p, "opp1"])

    def red_plain(s, p):
        a, b = first[p], second[p]
        for n in order:
            k = order.index(n)
            slot, place, to = (0, up, to_up) if n in high_names else (1, down, to_down)
            ub[s, p, 1 + slot, k] = mine_of(s, p, block(p, place[b], rels[n][a])).astype(BF16)
            send(ub.at[s, p, 1 + slot, k], vb_all.at[s, p, slot, k], to(b), ub_send, rb[s, p, (slot, "plain")])

    def red_sum(s, p):
        a, b = first[p], second[p]
        take(rb[s, p, "opp0"], vb_opp.at[s, p, pl.ds(0, 2)])
        take(rb[s, p, "opp1"], vb_opp.at[s, p, pl.ds(2, 2)])
        for n in order:
            k = order.index(n)
            slot, place, to = (0, up, to_up) if n in low_names else (1, down, to_down)
            value = mine_of(s, p, block(p, place[b], rels[n][a])) + vb_opp[s, p, k].astype(F32)
            ub[s, p, 1 + slot, k] = value.astype(BF16)
            send(ub.at[s, p, 1 + slot, k], vb_all.at[s, p, slot, k], to(b), ub_send, rb[s, p, (slot, "sum")])

    def line_sum(s, p, name):
        k = order.index(name)
        index = block(p, here[second[p]], rels[name][first[p]])
        return mine_of(s, p, index) + vb_all[s, p, 0, k].astype(F32) + vb_all[s, p, 1, k].astype(F32)

    def half_of(ref, k):
        return ref.at[:, pl.ds(k * HALF, HALF)]

    def red_line(s, p):
        a = first[p]
        for slot in range(2):
            for kind in ("plain", "sum"):
                take(rb[s, p, (slot, kind)], vb_all.at[s, p, slot, pl.ds(0, 2)])
        ua[s, p, 0] = line_sum(s, p, "opp").astype(BF16)
        send(half_of(ua.at[s, p, 0], 0), va_opp.at[s, p, 0], to_up(a), ua_send, ra[s, p, "opp0"])
        send(half_of(ua.at[s, p, 0], 1), va_opp.at[s, p, 1], to_down(a), ua_send, ra[s, p, "opp1"])
        for slot, name, to in ((0, "up", to_up), (1, "down", to_down)):
            value = line_sum(s, p, name)
            keep[s, p, slot] = value
            k = 1 - slot
            ua[s, p, 1 + slot, :, pl.ds(k * HALF, HALF)] = value[:, k * HALF : (k + 1) * HALF].astype(BF16)
            send(half_of(ua.at[s, p, 1 + slot], k), va_all.at[s, p, slot, k], to(a), ua_send, ra[s, p, (slot, "plain")])
        acc[s, p] = line_sum(s, p, "own")

    def red_line_sum(s, p):
        a = first[p]
        for slot, to in ((0, to_up), (1, to_down)):
            take(ra[s, p, f"opp{slot}"], va_opp.at[s, p, slot])
            value = keep[s, p, slot, :, pl.ds(slot * HALF, HALF)] + va_opp[s, p, slot].astype(F32)
            ua[s, p, 1 + slot, :, pl.ds(slot * HALF, HALF)] = value.astype(BF16)
            send(half_of(ua.at[s, p, 1 + slot], slot), va_all.at[s, p, slot, slot], to(a), ua_send, ra[s, p, (slot, "sum")])

    def red_end(s, p):
        for slot in range(2):
            for kind in ("plain", "sum"):
                take(ra[s, p, (slot, kind)], va_all.at[s, p, slot, 0])
        for k in range(2):
            acc[s, p, :, pl.ds(k * HALF, HALF)] += va_all[s, p, 0, k].astype(F32) + va_all[s, p, 1, k].astype(F32)

    def both(step, s):
        for p in range(2):
            step(s, p)

    row_recv = []

    def rows_step(s):
        for k in range(16):
            rows_out[s, :, k, :] = acc[s, k // 8, :, pl.ds((k % 8) * LANES, LANES)]
        rows_b[s] = rows_out[s].astype(BF16)
        ss, rr = new_send(rows_b.at[s, pl.ds(0, 15)]), new_recv()
        for dz, dc in column:
            z_, c_ = in_column(dz, dc)
            send(rows_b.at[s, z_ * 2 + c_], rows_in.at[s, c, z], device(x, y, z_, c_), ss, rr)
        rows_in[s, c, z] = jnp.zeros((16, LANES), BF16)
        row_recv.append(rr)

    for p in range(2):
        product(0, p)
        red_far(0, p)
        red_plain(0, p)
    for p in range(2):
        product(1, p)
        red_far(1, p)
    both(red_sum, 0)
    both(red_plain, 1)
    both(red_sum, 1)
    both(red_line, 0)
    both(red_line_sum, 0)
    both(red_end, 0)
    rows_step(0)
    both(red_line, 1)
    both(red_line_sum, 1)
    both(red_end, 1)
    rows_step(1)

    take(tt, stt2.at[pl.ds(0, 15)])
    target = jnp.sum(stt2[...], axis=0)
    place2 = lax.broadcasted_iota(jnp.int32, (2, LANES), 0) * LANES + lax.broadcasted_iota(jnp.int32, (2, LANES), 1)
    loss_ref[0, 0] = jnp.sum(jnp.where(place2 == spot * 16 + me, mx + jnp.log(total) - target, 0.0))

    for s in range(2):
        take(row_recv[s], rows_b.at[s, pl.ds(0, 15)])
        summed = jnp.sum(rows_in[s].astype(F32), axis=1)
        for half in range(2):
            row_f[pl.ds(half * 32 + s * 16, 16), :] = summed[half]
        row_f[pl.ds(pl.multiple_of(c * 32 + s * 16, 16), 16), :] += rows_out[s, me]
    row_f[...] = row_f[...] * lg_ref[0]
    for k in range(64):
        grad_ref[:, pl.ds(k * LANES, LANES)] = row_f[pl.ds(k, 1), :].astype(BF16)

    for sem, ref in ends:
        take(sem, ref)
    assert counts["send"] <= SENDS and counts["recv"] <= RECVS, counts


def shards(hidden, weight, targets, loss_grad):
    vmem = pltpu.VMEM
    loss, grad = pl.pallas_call(
        kernel,
        out_shape=(jax.ShapeDtypeStruct((1, 1), F32), jax.ShapeDtypeStruct((1, 8192), BF16)),
        in_specs=[
            pl.BlockSpec(memory_space=pltpu.VMEM),
            pl.BlockSpec(memory_space=pl.ANY),
            pl.BlockSpec(memory_space=pltpu.VMEM),
            pl.BlockSpec(memory_space=pltpu.SMEM),
        ],
        out_specs=(pl.BlockSpec(memory_space=pltpu.SMEM), pl.BlockSpec(memory_space=pltpu.VMEM)),
        scratch_shapes=[
            vmem((512, 8192), BF16),
            vmem((512, 4096), BF16),
            vmem((64, LANES), F32),
            vmem((64, LANES), BF16),
            vmem((2, 16, 16, LANES), BF16),
            vmem((16, 16, LANES), F32),
            vmem((4, 4, 4, 16, SLAB), BF16),
            vmem((512, 256), F32),
            vmem((512, 256), F32),
            vmem((2, 256, 512), BF16),
            vmem((2, 4, LANES), F32),
            vmem((16, 4, LANES), F32),
            vmem((16, 4, LANES), F32),
            vmem((2, 2, LANES), F32),
            vmem((16, 2, LANES), F32),
            vmem((16, 2, LANES), F32),
            vmem((2, 2, 4, 4, 16, PART), F32),
            vmem((2, 2, 3, 4, 16, PART), BF16),
            vmem((2, 2, 4, 16, PART), BF16),
            vmem((2, 2, 2, 4, 16, PART), BF16),
            vmem((2, 2, 2, 16, PART), F32),
            vmem((2, 2, 3, 16, PART), BF16),
            vmem((2, 2, 2, 16, HALF), BF16),
            vmem((2, 2, 2, 2, 16, HALF), BF16),
            vmem((2, 2, 16, PART), F32),
            vmem((2, 16, 16, LANES), F32),
            vmem((2, 16, 16, LANES), BF16),
            vmem((2, 2, 8, 16, LANES), BF16),
            pltpu.SemaphoreType.DMA((2,)),
            pltpu.SemaphoreType.DMA((SENDS,)),
            pltpu.SemaphoreType.DMA((RECVS,)),
        ],
        compiler_params=pltpu.CompilerParams(
            collective_id=0, has_side_effects=True, vmem_limit_bytes=60 * 1024 * 1024
        ),
    )(hidden, weight, targets.reshape(1, 256), loss_grad)
    return loss.reshape(1), grad


def solution(mesh):
    finer = Mesh(mesh.devices.reshape(4, 4, 2, 4, 2), AXES)
    return jax.shard_map(
        shards,
        mesh=finer,
        in_specs=(P(AXES, None), P(AXES, None), P(), P(AXES)),
        out_specs=(P(AXES), P(AXES, None)),
        check_vma=False,
    )
```

```python
import jax
import jax.numpy as jnp
from jax import lax
from jax.experimental import pallas as pl
from jax.experimental.pallas import tpu as pltpu
from jax.sharding import Mesh
from jax.sharding import PartitionSpec as P

AXES = ("zl", "x", "zh", "y", "c")
F32, BF16 = jnp.float32, jnp.bfloat16
PART = 2048
LANES = 128
TURN = 1024
SENDS, RECVS = 16, 68
MESH = pl.DeviceIdType.MESH


def kernel(
    h_hbm, w_hbm, tgt_hbm, lg_ref, loss_ref, grad_ref,
    h_ref, tgt_ref, wt, part_logits,
    wv, wp, row_f, row_b, got, wide, hid, logits, logits_p, pt, stz, stz1, stz2,
    own_sum, ub, vb_opp, vb_all, ua, va, acc, rows_out, rows_b, rows_in,
    w_sem, send_sem, recv_sem,
):
    zl, x, zh, y, c = (lax.axis_index(a) for a in AXES)
    z = zh * 4 + zl
    me, spot = z * 2 + c, y * 4 + x
    counts = {"send": 0, "recv": 0}
    ends = []

    def new(kind, sem):
        counts[kind] += 1
        return sem.at[counts[kind] - 1]

    def new_recv():
        return new("recv", recv_sem)

    def new_send(ref):
        s = new("send", send_sem)
        ends.append((s, ref))
        return s

    def take(sem, ref):
        pltpu.make_async_copy(ref, ref, sem).wait()

    def send(src, dst, to, s, r):
        pltpu.make_async_remote_copy(
            src_ref=src, dst_ref=dst, send_sem=s, recv_sem=r, device_id=to, device_id_type=MESH
        ).start()

    def device(x_, y_, z_, c_):
        return (lax.rem(z_, 4), x_, lax.div(z_, 4), y_, c_)

    up = {"x": lax.rem(x + 1, 4), "y": lax.rem(y + 1, 4)}
    opp = {"x": lax.rem(x + 2, 4), "y": lax.rem(y + 2, 4)}
    down = {"x": lax.rem(x + 3, 4), "y": lax.rem(y + 3, 4)}
    here = {"x": x, "y": y}
    rels = {"own": here, "down": down, "up": up, "opp": opp}
    first, second = ("x", "y"), ("y", "x")
    order = ("own", "up", "down", "opp")

    def to_up(axis):
        return device(up["x"] if axis == "x" else x, up["y"] if axis == "y" else y, z, c)

    def to_opp(axis):
        return device(opp["x"] if axis == "x" else x, opp["y"] if axis == "y" else y, z, c)

    def to_down(axis):
        return device(down["x"] if axis == "x" else x, down["y"] if axis == "y" else y, z, c)

    partner = device(x, y, z, 1 - c)
    column = [(dz, dc) for dz in (4, 3, 5, 2, 6, 1, 7, 0) for dc in range(2) if (dz, dc) != (0, 0)]
    plane = [(dx, dy) for dx in (2, 1, 3, 0) for dy in (2, 1, 3, 0) if (dx, dy) != (0, 0)]

    def in_column(dz, dc):
        return lax.rem(z + dz, 8), lax.rem(c + dc, 2)

    def in_plane(dx, dy):
        return lax.rem(x + dx, 4), lax.rem(y + dy, 4)

    def block(part, b_index, a_index):
        return (b_index, a_index) if part == 0 else (a_index, b_index)

    barrier = pltpu.get_barrier_semaphore()
    for dz, dc in column:
        z_, c_ = in_column(dz, dc)
        pl.semaphore_signal(barrier, inc=1, device_id=device(x, y, z_, c_), device_id_type=MESH)
    for dx, dy in plane:
        x_, y_ = in_plane(dx, dy)
        pl.semaphore_signal(barrier, inc=1, device_id=device(x_, y_, z, c), device_id_type=MESH)

    small = [pltpu.make_async_copy(h_hbm, h_ref, w_sem.at[2]), pltpu.make_async_copy(tgt_hbm, tgt_ref, w_sem.at[3])]
    for copy in small:
        copy.start()
    halfway = PART * 2
    w_copies = []
    for k, half in enumerate((1 - c, c)):
        cols = pl.ds(pl.multiple_of(half * halfway, halfway), halfway)
        w_copies.append(pltpu.make_async_copy(w_hbm.at[:, cols], wv.at[:, cols], w_sem.at[k]))
        w_copies[-1].start()

    for copy in small:
        copy.wait()

    for k in range(64):
        row_f[pl.ds(k, 1), :] = h_ref[:, pl.ds(k * LANES, LANES)].astype(F32)
    row_b[...] = row_f[...].astype(BF16)

    chip_base = ((zl * 4 + x) * 16 + zh * 8 + y * 2) * 512
    rel = tgt_ref[...] - chip_base
    near = jnp.logical_and(rel >= 0, rel < 1024)
    high = jnp.where(near, lax.shift_right_logical(rel, 4), 128)
    low = jnp.where(near, jnp.bitwise_and(rel, 15), 0)
    digit = lax.broadcasted_iota(jnp.int32, (16, 256), 0)
    digits = jnp.where(digit == 0, high, jnp.where(digit == 1, low, 0)).astype(F32).astype(BF16)
    r = lax.broadcasted_iota(jnp.int32, (256, 256), 1)
    t = lax.broadcasted_iota(jnp.int32, (256, 256), 0)
    bits = jnp.bitwise_and
    shift = lax.shift_right_logical
    token = (
        bits(shift(r, 1), 3) * 64 + bits(shift(r, 3), 3) * 16 + shift(r, 7) * 8 + bits(shift(r, 5), 3) * 2 + bits(r, 1)
    )
    moves = jnp.where(t == token, 1.0, 0.0).astype(BF16)
    placed = jnp.dot(digits, moves, preferred_element_type=F32)
    chip_row = (placed[0:1] * 16.0 + placed[1:2]).astype(jnp.int32)

    pl.semaphore_wait(barrier, len(column) + len(plane))

    ss, both_recv = new_send(got.at[pl.ds(0, 15)]), [new_recv(), new_recv()]
    base = counts["recv"] - 2
    for dz, dc in column:
        z_, c_ = in_column(dz, dc)
        rows = pl.ds(pl.multiple_of(c_ * 32, 32), 32)
        send(row_b.at[rows], got.at[me], device(x, y, z_, c_), ss, recv_sem.at[base + zh])
    rows = pl.ds(pl.multiple_of(c * 32, 32), 32)
    pltpu.make_async_copy(row_b.at[rows], got.at[me], recv_sem.at[base + zh]).start()

    a_send = new_send(hid.at[0, 0, pl.ds(0, 3), pl.ds(0, 2)])
    not_own = ("down", "up", "opp")
    b_send = new_send(hid.at[0, pl.ds(0, 2), pl.ds(0, 3)])
    share_send = new_send(hid.at[0])
    share_recv = [new_recv() for _ in range(2)]
    w_send, w_recv = new_send(wp), new_recv()
    a_recv = {(s, p): new_recv() for s in range(2) for p in range(2)}
    b_recv = {
        (s, p, side, k): new_recv()
        for s in range(2) for p in range(2) for side in ("down", "up") for k in ("own", "rest", "far")
    }

    def blk(s, p, index):
        return hid.at[s, c, index[0], index[1], :, pl.ds(p * PART, PART)]

    def share(s, p, index):
        ref = blk(s, p, index)
        send(ref, ref, partner, share_send, share_recv[s])

    def w_piece(k):
        src = wv.at[pl.ds(64 * k, 64), pl.ds(pl.multiple_of((1 - c) * halfway, halfway), halfway)]
        send(src, wp.at[pl.ds(64 * k, 64)], partner, w_send, w_recv)

    def second_axis(s, p, name, group):
        b = second[p]
        index = block(p, here[b], rels[name][first[p]])
        ref = blk(s, p, index)
        send(ref, ref, to_up(b), b_send, b_recv[s, p, "down", group])
        send(ref, ref, to_down(b), b_send, b_recv[s, p, "up", group])
        share(s, p, index)

    def step_c(s):
        take(both_recv[s], got.at[pl.ds(0, 8)])
        wide[...] = got[pl.ds(8 * s, 8)].astype(F32)
        for k in range(32):
            hid[s, c, y, x, :, pl.ds(k * LANES, LANES)] = wide[:, k, :].astype(BF16)
        for p in range(2):
            a = first[p]
            ref = blk(s, p, (y, x))
            for to in (to_up, to_down, to_opp):
                send(ref, ref, to(a), a_send, a_recv[s, p])
        for p in range(2):
            second_axis(s, p, "own", "own")

    def step_a(s):
        for p in range(2):
            take(a_recv[s, p], hid.at[s, 0, 0, pl.ds(0, 3), :, pl.ds(0, PART)])
            for name in not_own:
                second_axis(s, p, name, "rest")

    def step_b(s, group):
        names = {"own": ("own",), "rest": not_own}[group]
        for p in range(2):
            a, b = first[p], second[p]
            for side, place, to in (("down", down, to_up), ("up", up, to_down)):
                refs = [(n, block(p, place[b], rels[n][a])) for n in names]
                some = hid.at[s, 0, 0, pl.ds(0, len(names)), :, pl.ds(0, PART)]
                take(b_recv[s, p, side, group], some)
                for n, index in refs:
                    if (n in ("own", "up")) == (side == "down"):
                        ref = blk(s, p, index)
                        send(ref, ref, to(b), b_send, b_recv[s, p, side, "far"])
                for n, index in refs:
                    share(s, p, index)

    def step_far(s):
        for p in range(2):
            a, b = first[p], second[p]
            for side, names in (("down", ("own", "up")), ("up", ("down", "opp"))):
                take(b_recv[s, p, side, "far"], hid.at[s, 0, 0, pl.ds(0, 2), :, pl.ds(0, PART)])
                for n in names:
                    share(s, p, block(p, opp[b], rels[n][a]))

    def turn(n):
        def piece(k, _):
            at = pl.ds(pl.multiple_of(n * TURN + k * 256, 256), 256)
            wt[at, :] = wv[:, at].T
            return 0

        lax.fori_loop(0, TURN // 256, piece, 0)

    def step_logits(s, half, start=False):
        part = jnp.dot(
            hid[s, half].reshape(128, halfway),
            wt[pl.ds(pl.multiple_of(half * halfway, halfway), halfway), :],
            preferred_element_type=F32,
        )
        if start:
            part_logits[...] = part
        else:
            logits[s] = (part_logits[...] + part).T

    vocab_row = lax.broadcasted_iota(jnp.int32, (512, 128), 0)
    chunk_row = [chip_row[:, s * 128 : (s + 1) * 128] for s in range(2)]
    swap_send = new_send(logits)
    swap_recv = [new_recv() for _ in range(2)]
    stat_recv = {}

    def stat_local(s):
        send(logits.at[s], logits_p.at[s], partner, swap_send, swap_recv[s])
        lt = logits[s]
        mask = vocab_row + c * 512 == chunk_row[s]
        local_max = jnp.max(lt, axis=0, keepdims=True)
        stz[s, 0, pl.ds(0, 1), :] = local_max
        stz[s, 0, pl.ds(1, 1), :] = jnp.sum(jnp.exp(lt - local_max), axis=0, keepdims=True)
        stz[s, 0, pl.ds(2, 1), :] = jnp.sum(jnp.where(mask, lt, 0.0), axis=0, keepdims=True)
        ss, stat_recv[s, 0] = new_send(stz1.at[s, pl.ds(0, 15)]), new_recv()
        for dz, dc in column:
            z_, c_ = in_column(dz, dc)
            send(stz.at[s, 0], stz1.at[s, me], device(x, y, z_, c_), ss, stat_recv[s, 0])
        stz1[s, me] = stz[s, 0]

    def combined(v):
        mx = jnp.max(v[:, 0:1], axis=0)
        total = jnp.sum(v[:, 1:2] * jnp.exp(v[:, 0:1] - mx[None]), axis=0)
        return mx, total, jnp.sum(v[:, 2:3], axis=0)

    def stat_column(s):
        take(stat_recv[s, 0], stz1.at[s, pl.ds(0, 15)])
        for k, v in enumerate(combined(stz1[s])):
            stz[s, 1, pl.ds(k, 1), :] = v
        ss, stat_recv[s, 1] = new_send(stz2.at[s, pl.ds(0, 15)]), new_recv()
        for dx, dy in plane:
            x_, y_ = in_plane(dx, dy)
            send(stz.at[s, 1], stz2.at[s, spot], device(x_, y_, z, c), ss, stat_recv[s, 1])
        stz2[s, spot] = stz[s, 1]

    def probs(s):
        take(stat_recv[s, 1], stz2.at[s, pl.ds(0, 15)])
        take(swap_recv[s], logits_p.at[s])
        mx, total, target = combined(stz2[s])
        column_id = lax.broadcasted_iota(jnp.int32, (1, LANES), 1)
        chosen = jnp.logical_and(column_id == spot * 8 + zl * 2 + c, zh == s)
        loss = jnp.sum(jnp.where(chosen, mx + jnp.log(total) - target, 0.0))
        inverse = 1.0 / total
        for k, (ref, half) in enumerate(((logits, c), (logits_p, 1 - c))):
            mask = vocab_row + half * 512 == chunk_row[s]
            value = jnp.exp(ref[s] - mx) * inverse - jnp.where(mask, 1.0, 0.0)
            pt[s, k] = value.T.astype(BF16)
        return loss

    low_names, high_names = ("own", "up"), ("down", "opp")
    ub_send, ua_send = new_send(ub), new_send(ua)
    rb = {
        (s, p, k): new_recv() for s in range(2) for p in range(2)
        for k in ("opp0", "opp1", (0, "plain"), (0, "sum"), (1, "plain"), (1, "sum"))
    }
    ra = {(s, p): new_recv() for s in range(2) for p in range(2)}

    def product(s, p):
        mine = pl.ds(pl.multiple_of(c * halfway + p * PART, PART), PART)
        theirs = pl.ds(p * PART, PART)
        out = jnp.dot(pt[s, 0], wv[:, mine], preferred_element_type=F32) + jnp.dot(
            pt[s, 1], wp[:, theirs], preferred_element_type=F32
        )
        own_sum[s, p] = out.reshape(4, 4, 8, PART)

    def mine_of(s, p, index):
        return own_sum[s, p, index[0], index[1]]

    def red_far(s, p):
        a, b = first[p], second[p]
        for n in order:
            k = order.index(n)
            ub[s, p, 0, k] = mine_of(s, p, block(p, opp[b], rels[n][a])).astype(BF16)
            if n in low_names:
                send(ub.at[s, p, 0, k], vb_opp.at[s, p, k], to_up(b), ub_send, rb[s, p, "opp0"])
            else:
                send(ub.at[s, p, 0, k], vb_opp.at[s, p, k], to_down(b), ub_send, rb[s, p, "opp1"])

    def red_plain(s, p):
        a, b = first[p], second[p]
        for n in order:
            k = order.index(n)
            slot, place, to = (0, up, to_up) if n in high_names else (1, down, to_down)
            ub[s, p, 1 + slot, k] = mine_of(s, p, block(p, place[b], rels[n][a])).astype(BF16)
            send(ub.at[s, p, 1 + slot, k], vb_all.at[s, p, slot, k], to(b), ub_send, rb[s, p, (slot, "plain")])

    def red_sum(s, p):
        a, b = first[p], second[p]
        take(rb[s, p, "opp0"], vb_opp.at[s, p, pl.ds(0, 2)])
        take(rb[s, p, "opp1"], vb_opp.at[s, p, pl.ds(2, 2)])
        for n in order:
            k = order.index(n)
            slot, place, to = (0, up, to_up) if n in low_names else (1, down, to_down)
            value = mine_of(s, p, block(p, place[b], rels[n][a])) + vb_opp[s, p, k].astype(F32)
            ub[s, p, 1 + slot, k] = value.astype(BF16)
            send(ub.at[s, p, 1 + slot, k], vb_all.at[s, p, slot, k], to(b), ub_send, rb[s, p, (slot, "sum")])

    def line_sum(s, p, name):
        k = order.index(name)
        index = block(p, here[second[p]], rels[name][first[p]])
        return mine_of(s, p, index) + vb_all[s, p, 0, k].astype(F32) + vb_all[s, p, 1, k].astype(F32)

    def red_line(s, p):
        a = first[p]
        for slot in range(2):
            for kind in ("plain", "sum"):
                take(rb[s, p, (slot, kind)], vb_all.at[s, p, slot, pl.ds(0, 2)])
        for k, (name, to) in enumerate((("opp", to_opp), ("up", to_up), ("down", to_down))):
            ua[s, p, k] = line_sum(s, p, name).astype(BF16)
            send(ua.at[s, p, k], va.at[s, p, k], to(a), ua_send, ra[s, p])
        acc[s, p] = line_sum(s, p, "own")

    def red_end(s, p):
        take(ra[s, p], va.at[s, p])
        acc[s, p] += jnp.sum(va[s, p].astype(F32), axis=0)

    def both(step, s):
        for p in range(2):
            step(s, p)

    row_recv, row_send, last_send = new_recv(), [], []

    def rows_step(s):
        for k in range(32):
            rows_out[:, k, :] = acc[s, k // 16, :, pl.ds((k % 16) * LANES, LANES)]
        rows_b[s] = rows_out[...].astype(BF16)
        ss = new_send(rows_b.at[s, pl.ds(0, 7)])
        counts["send"] += 1
        straight = send_sem.at[counts["send"] - 1]
        for dz in (2, 1, 3, 0):
            for dc in (1, 0):
                zl_, c_ = lax.rem(zl + dz, 4), lax.rem(c + dc, 2)
                src, dst = rows_b.at[s, zl_ * 2 + c_], rows_in.at[c, z]
                to = device(x, y, zl_ + 4 * s, c_)
                if dz or dc:
                    send(src, dst, to, ss, row_recv)
                else:

                    @pl.when(zh == s)
                    def _(src=src, dst=dst):
                        pltpu.make_async_copy(src, dst, row_recv).start()

                    @pl.when(zh != s)
                    def _(src=src, dst=dst, to=to):
                        send(src, dst, to, straight, row_recv)

        last_send.append((s, straight))

    w_copies[0].wait()
    for n in range(4):
        turn((1 - c) * 4 + n)
    w_copies[1].wait()
    for n in range(4):
        turn(c * 4 + n)
    step_c(0)
    step_c(1)
    w_piece(0)
    w_piece(1)
    step_a(0)
    step_b(0, "own")
    w_piece(2)
    step_a(1)
    w_piece(3)
    step_b(0, "rest")
    w_piece(4)
    step_b(1, "own")
    w_piece(5)
    step_far(0)
    w_piece(6)
    step_logits(0, c, True)
    step_b(1, "rest")
    w_piece(7)
    take(share_recv[0], hid.at[0, 0])
    step_logits(0, 1 - c)
    stat_local(0)
    step_far(1)
    step_logits(1, c, True)
    take(share_recv[1], hid.at[0, 0])
    step_logits(1, 1 - c)
    stat_local(1)
    stat_column(0)
    take(w_recv, wp)
    loss = probs(0)
    for p in range(2):
        product(0, p)
        red_far(0, p)
        red_plain(0, p)
    stat_column(1)
    both(red_sum, 0)
    loss += probs(1)
    loss_ref[0, 0] = loss
    for p in range(2):
        product(1, p)
        red_far(1, p)
    both(red_plain, 1)
    both(red_line, 0)
    both(red_sum, 1)
    both(red_end, 0)
    rows_step(0)
    both(red_line, 1)
    both(red_end, 1)
    rows_step(1)

    take(row_recv, rows_in)
    row_f[...] = jnp.sum(rows_in[...].astype(F32), axis=1).reshape(64, LANES) * lg_ref[0]
    for k in range(64):
        grad_ref[:, pl.ds(k * LANES, LANES)] = row_f[pl.ds(k, 1), :].astype(BF16)

    for s, sem in last_send:

        @pl.when(zh != s)
        def _(s=s, sem=sem):
            take(sem, rows_b.at[s, 0])

    for sem, ref in ends:
        take(sem, ref)
    assert counts == {"send": SENDS, "recv": RECVS}, counts


def shards(hidden, weight, targets, loss_grad):
    vmem = pltpu.VMEM
    loss, grad = pl.pallas_call(
        kernel,
        out_shape=(jax.ShapeDtypeStruct((1, 1), F32), jax.ShapeDtypeStruct((1, 8192), BF16)),
        in_specs=[
            pl.BlockSpec(memory_space=pl.ANY),
            pl.BlockSpec(memory_space=pl.ANY),
            pl.BlockSpec(memory_space=pl.ANY),
            pl.BlockSpec(memory_space=pltpu.SMEM),
        ],
        out_specs=(pl.BlockSpec(memory_space=pltpu.SMEM), pl.BlockSpec(memory_space=pltpu.VMEM)),
        scratch_shapes=[
            vmem((1, 8192), BF16),
            vmem((1, 256), jnp.int32),
            vmem((8192, 512), BF16),
            vmem((128, 512), F32),
            vmem((512, 8192), BF16),
            vmem((512, 4096), BF16),
            vmem((64, LANES), F32),
            vmem((64, LANES), BF16),
            vmem((16, 32, LANES), BF16),
            vmem((8, 32, LANES), F32),
            vmem((2, 2, 4, 4, 8, 2 * PART), BF16),
            vmem((2, 512, LANES), F32),
            vmem((2, 512, LANES), F32),
            vmem((2, 2, 128, 512), BF16),
            vmem((2, 2, 3, LANES), F32),
            vmem((2, 16, 3, LANES), F32),
            vmem((2, 16, 3, LANES), F32),
            vmem((2, 2, 4, 4, 8, PART), F32),
            vmem((2, 2, 3, 4, 8, PART), BF16),
            vmem((2, 2, 4, 8, PART), BF16),
            vmem((2, 2, 2, 4, 8, PART), BF16),
            vmem((2, 2, 3, 8, PART), BF16),
            vmem((2, 2, 3, 8, PART), BF16),
            vmem((2, 2, 8, PART), F32),
            vmem((8, 32, LANES), F32),
            vmem((2, 8, 32, LANES), BF16),
            vmem((2, 8, 32, LANES), BF16),
            pltpu.SemaphoreType.DMA((4,)),
            pltpu.SemaphoreType.DMA((SENDS,)),
            pltpu.SemaphoreType.DMA((RECVS,)),
        ],
        compiler_params=pltpu.CompilerParams(
            collective_id=0, has_side_effects=True, vmem_limit_bytes=60 * 1024 * 1024
        ),
    )(hidden, weight, targets.reshape(1, 256), loss_grad)
    return loss.reshape(1), grad


def solution(mesh):
    finer = Mesh(mesh.devices.reshape(4, 4, 2, 4, 2), AXES)
    return jax.shard_map(
        shards,
        mesh=finer,
        in_specs=(P(AXES, None), P(AXES, None), P(), P(AXES)),
        out_specs=(P(AXES), P(AXES, None)),
        check_vma=False,
    )
```
